1024 devices in a mesh: ctx: 128 (over z, y), head: 8 (over x, core).
Axes of the slice: x: 4, y: 8, z: 16, core: 2. Of those that a mesh axis runs over, the one named last changes fastest.
Arguments:
- queries: bfloat16 [65536, 4096], P('ctx', 'head'), may hold values from -8 to 8
- keys: bfloat16 [65536, 1024], P('ctx', 'head'), may hold values from -8 to 8
- values: bfloat16 [65536, 1024], P('ctx', 'head'), may hold values from -6 to 6
- output_gradient: bfloat16 [65536, 4096], P('ctx', 'head'), may hold values from -6 to 6
- blocks: int32 [512, 8], P('ctx'), may hold values from 0 to 511, as said below
- counts: int32 [512], P('ctx'), may hold values from 2 to 8, as said below
Outputs:
- dqueries: bfloat16 [65536, 4096], P(('ctx', 'head'))
- dkeys: bfloat16 [65536, 1024], P(('ctx', 'head'))
- dvalues: bfloat16 [65536, 1024], P(('ctx', 'head'))
The draws below stay inside these ranges and needn't reach their ends.
Inputs may be any that keep to these rules, and one draw needn't show every extreme that they name: For the query block b on token shard i = b // 4, all 8 entries of row b are distinct and name key blocks of the shards i - 2 to i + 2, taken around the closed cycle of 512 blocks. `counts`: some rows have all 8 entries live.
All inputs are finite; a program needn't handle non-finite values.
Results may differ from the reference program's by a relative error of at most 0.0088.
Values may be sent and summed in bfloat16 or wider, within the bound.
A program may use at most 32 MiB of HBM per device.

```python
import math
import jax
import jax.numpy as jnp
from jax import lax

HEAD_SIZE = 128
QUERY_HEADS = 32
KEY_VALUE_HEADS = 8
BLOCK_TOKENS = 128
SLOTS = 8
REACH = 2
ARRAY_TOKENS = 65536
QB_DEV = 4
QUERY_BLOCKS = 512


def draw_queries(key, part):
    final_gradients = jnp.clip(jax.random.normal(jax.random.fold_in(key, 19), (ARRAY_TOKENS, QUERY_HEADS, HEAD_SIZE), jnp.float32), -6.0, 6.0)
    return final_gradients.reshape(ARRAY_TOKENS, QUERY_HEADS * HEAD_SIZE).astype(jnp.bfloat16)


def draw_keys(key, part):
    final_gradients = jnp.clip(jax.random.normal(jax.random.fold_in(key, 29), (ARRAY_TOKENS, KEY_VALUE_HEADS, HEAD_SIZE), jnp.float32), -6.0, 6.0)
    return final_gradients.reshape(ARRAY_TOKENS, KEY_VALUE_HEADS * HEAD_SIZE).astype(jnp.bfloat16)


def draw_blocks(key, part):
    window_size = (2 * REACH + 1) * QB_DEV
    subkeys = jax.random.split(jax.random.fold_in(key, 11), QUERY_BLOCKS)

    def pick_slots(subkey):
        return jax.random.permutation(subkey, window_size)[:SLOTS]
    chosen = jax.vmap(pick_slots)(subkeys).astype(jnp.int32)
    positions = jnp.arange(QUERY_BLOCKS, dtype=jnp.int32)
    window_start = (positions // QB_DEV - REACH) * QB_DEV
    return jnp.mod(window_start[:, None] + chosen, QUERY_BLOCKS).astype(jnp.int32)


def draw_counts(key, part):
    drawn = jax.random.randint(jax.random.fold_in(key, 13), (QUERY_BLOCKS,), 2, SLOTS + 1)
    positions = jnp.arange(QUERY_BLOCKS, dtype=jnp.int32)
    drawn = jnp.where(positions % 5 == 0, SLOTS, drawn)
    drawn = jnp.where(positions % 7 == 3, 2, drawn)
    return drawn.astype(jnp.int32)


def block_levels(stream_key, dims, cuts, least, high):
    gain, own = 1.0, jax.random.fold_in(stream_key, 6)
    for dim, parts in cuts:
        draws = jnp.exp(jax.random.uniform(jax.random.fold_in(own, dim), (parts,), jnp.float32, least / len(cuts), high / len(cuts)))
        gain = gain * jnp.repeat(draws, dims[dim] // parts).reshape([-1 if axis == dim else 1 for axis in range(len(dims))])
    return gain


def bell_draw(stream_key, dims, width, most, pieces=(), held_as=jnp.bfloat16):
    values = jax.random.normal(stream_key, dims, jnp.float32) * width
    if len(pieces) > 0:
        values = block_levels(stream_key, dims, pieces, -0.22, 0.18) * values
    return jnp.clip(values, min=-most, max=most).astype(held_as)


def setup_inputs(seed: int = 0) -> dict:
    key_of = jax.random.split(jax.random.key(seed), 7)
    return {
        "queries": draw_queries(jax.random.fold_in(key_of[6], 71), 0),
        "keys": draw_keys(jax.random.fold_in(key_of[6], 71), 0),
        "values": bell_draw(key_of[2], (ARRAY_TOKENS, KEY_VALUE_HEADS * HEAD_SIZE), 1.0, 6.0, ((0, 128), (1, 8))),
        "output_gradient": bell_draw(key_of[3], (ARRAY_TOKENS, QUERY_HEADS * HEAD_SIZE), 1.0, 6.0, ((0, 128), (1, 8))),
        "blocks": draw_blocks(jax.random.fold_in(key_of[6], 71), 0),
        "counts": draw_counts(jax.random.fold_in(key_of[6], 71), 0),
    }


def reference(queries, keys, values, output_gradient, blocks, counts):
    query_group = QUERY_HEADS // KEY_VALUE_HEADS
    softmax_scale = 1.0 / math.sqrt(HEAD_SIZE)
    blocked_queries = queries.reshape(QUERY_BLOCKS, BLOCK_TOKENS, KEY_VALUE_HEADS, query_group, HEAD_SIZE)
    output_blocks = output_gradient.reshape(QUERY_BLOCKS, BLOCK_TOKENS, KEY_VALUE_HEADS, query_group, HEAD_SIZE)
    blocked_keys = keys.reshape(QUERY_BLOCKS, BLOCK_TOKENS, KEY_VALUE_HEADS, HEAD_SIZE)
    blocked_values = values.reshape(QUERY_BLOCKS, BLOCK_TOKENS, KEY_VALUE_HEADS, HEAD_SIZE)

    def qblock_step(running, qblock):
        key_gradient_sum, value_gradient_sum = running
        slot_blocks = blocks[qblock]
        live_slots = jnp.arange(SLOTS) < counts[qblock]
        live_mask = live_slots[None, None, None, :, None]
        kblock = blocked_keys[slot_blocks].astype(jnp.float32)
        vblock = blocked_values[slot_blocks].astype(jnp.float32)
        qrows = blocked_queries[qblock].astype(jnp.float32)
        orows = output_blocks[qblock].astype(jnp.float32)
        scores = jnp.einsum('rhgd,schd->hgrsc', qrows, kblock) * softmax_scale
        scores = jnp.where(live_mask, scores, -1e+30)
        row_max = lax.optimization_barrier(jnp.max(scores, axis=(3, 4), keepdims=True))
        weights = jnp.where(live_mask, jnp.exp(scores - row_max), 0.0)
        probs = weights / lax.optimization_barrier(jnp.sum(weights, axis=(3, 4), keepdims=True))
        dprobs = jnp.einsum('rhgd,schd->hgrsc', orows, vblock)
        row_delta = lax.optimization_barrier(jnp.sum(probs * dprobs, axis=(3, 4), keepdims=True))
        dscores = lax.optimization_barrier((probs * (dprobs - row_delta)).astype(jnp.bfloat16)).astype(jnp.float32)
        probs_bf = lax.optimization_barrier(probs.astype(jnp.bfloat16)).astype(jnp.float32)
        dquery = softmax_scale * jnp.einsum('hgrsc,schd->rhgd', dscores, kblock)
        dkey_part = softmax_scale * jnp.einsum('hgrsc,rhgd->schd', dscores, qrows)
        dvalue_part = jnp.einsum('hgrsc,rhgd->schd', probs_bf, orows)
        key_gradient_sum = key_gradient_sum.at[slot_blocks].add(dkey_part)
        value_gradient_sum = value_gradient_sum.at[slot_blocks].add(dvalue_part)
        return ((key_gradient_sum, value_gradient_sum), dquery.astype(jnp.bfloat16).reshape(BLOCK_TOKENS, QUERY_HEADS * HEAD_SIZE))
    empty_gradient = jnp.zeros((QUERY_BLOCKS, BLOCK_TOKENS, KEY_VALUE_HEADS, HEAD_SIZE), jnp.float32)
    (key_gradient_sum, value_gradient_sum), dquery_rows = lax.scan(qblock_step, (empty_gradient, empty_gradient), jnp.arange(QUERY_BLOCKS, dtype=jnp.int32))
    dqueries = dquery_rows.reshape(ARRAY_TOKENS, QUERY_HEADS * HEAD_SIZE)
    dkeys = key_gradient_sum.reshape(ARRAY_TOKENS, KEY_VALUE_HEADS * HEAD_SIZE).astype(jnp.bfloat16)
    dvalues = value_gradient_sum.reshape(ARRAY_TOKENS, KEY_VALUE_HEADS * HEAD_SIZE).astype(jnp.bfloat16)
    return (dqueries, dkeys, dvalues)
```

```python
import functools
import math

import jax
import jax.numpy as jnp
from jax import lax
from jax.experimental import pallas as pl
from jax.experimental.pallas import tpu as pltpu
from jax.sharding import PartitionSpec as P

D = 128
BT = 128
SLOTS = 8
REACH = 2
SEGS = 2 * REACH + 1
CHUNKS = 2
MESH = pl.DeviceIdType.MESH
F32 = jnp.float32
BF16 = jnp.bfloat16


def nt(a, b):
    return lax.dot_general(a, b, (((1,), (1,)), ((), ())), preferred_element_type=F32)


def nn(a, b):
    return lax.dot_general(a, b, (((1,), (0,)), ((), ())), preferred_element_type=F32)


def tn(a, b):
    return lax.dot_general(a, b, (((0,), (0,)), ((), ())), preferred_element_type=F32)


def kernel(
    n_ctx, n_head, tok, group,
    q_ref, k_ref, v_ref, do_ref, table, live,
    dq_out, dk_out, dv_out,
    k_win, v_win, kg, st, wb, dop, invs, dvp, dkp, dq_buf,
    v_send1, v_recv1, v_send2, v_recv2, k_send1, k_recv1, k_send2, k_recv2,
    fin_v, fin_k, dq_land, dk_land, dv_land,
    win_ss, win_rs, red_ss, red_rs, ex_ss, ex_rs,
):
    nq = tok // BT
    nw = SEGS * nq
    rows = tok // n_head
    chunk = tok // CHUNKS
    cb = chunk // BT
    me = lax.axis_index("ctx")
    h = lax.axis_index("head")
    ahead = lax.rem(me + 1, n_ctx)
    behind = lax.rem(me + n_ctx - 1, n_ctx)
    to = (ahead, behind)
    scale = 1.0 / math.sqrt(D)
    c2 = scale * math.log2(math.e)

    def remote(src, dst, ss, rs, dev):
        return pltpu.make_async_remote_copy(
            src_ref=src, dst_ref=dst, send_sem=ss, recv_sem=rs, device_id=dev, device_id_type=MESH
        )

    barrier = pltpu.get_barrier_semaphore()
    for d in range(2):
        pl.semaphore_signal(barrier, inc=1, device_id={"ctx": to[d]}, device_id_type=MESH)
    for t in range(1, n_head):
        pl.semaphore_signal(
            barrier, inc=1, device_id={"head": lax.rem(h + t, n_head)}, device_id_type=MESH
        )
    pl.semaphore_wait(barrier, 2 + n_head - 1)

    near, far = (1, 3), (0, 4)

    def win(a, hop, d, c):
        ref, window = ((k_ref, k_win), (v_ref, v_win))[a]
        if hop == 0:
            src = ref.at[pl.ds(c * cb, cb)]
            seg = near[d]
        else:
            src = window.at[pl.ds(near[d] * nq + c * cb, cb)]
            seg = far[d]
        dst = window.at[pl.ds(seg * nq + c * cb, cb)]
        return remote(src, dst, win_ss.at[a, hop, d, c], win_rs.at[a, hop, d, c], {"ctx": to[d]})

    both = [(c, d) for c in range(CHUNKS) for d in range(2)]
    for c, d in both:
        win(0, 0, d, c).start()

    k_win[pl.ds(REACH * nq, nq)] = k_ref[...]
    v_win[pl.ds(REACH * nq, nq)] = v_ref[...]
    k_win[nw] = jnp.zeros((BT, D), BF16)
    v_win[nw] = jnp.zeros((BT, D), BF16)
    for qb in range(nq):
        dvp[qb, SLOTS] = jnp.zeros((BT, D), F32)
        dkp[qb, SLOTS] = jnp.zeros((BT, D), F32)

    for c, d in both:
        win(0, 0, d, c).wait_recv()
        win(0, 1, d, c).start()
    for c, d in both:
        win(1, 0, d, c).start()
    for c, d in both:
        win(0, 1, d, c).wait_recv()

    def stack_heads(ref, qb):
        r = pl.ds(pl.multiple_of(qb * BT, BT), BT)
        return jnp.concatenate([ref[r, g * D:(g + 1) * D] for g in range(group)], axis=0)

    def gather_blocks(window, first, qb):
        for s in range(SLOTS):
            kg[pl.ds(s * BT, BT), :] = window[table[qb, first + s]]

    width = group * BT

    def probs_step(qb, carry):
        for c in range(CHUNKS):
            @pl.when(qb == c + 1)
            def _():
                for d in range(2):
                    win(1, 0, d, c).wait_recv()
                    win(1, 1, d, c).start()
        qs = stack_heads(q_ref, qb)
        gather_blocks(k_win, 0, qb)
        st[...] = nt(kg[...], qs)
        top = jnp.max(st[...], axis=0, keepdims=True) * c2
        total = jnp.zeros((1, width), F32)
        for s in range(SLOTS):
            w = jnp.exp2(st[pl.ds(s * BT, BT), :] * c2 - top).astype(BF16)
            part = jnp.sum(w.astype(F32), axis=0, keepdims=True)
            total = total + part * live[qb, s]
            wb[qb, pl.ds(s * BT, BT), :] = w
        norm = 1.0 / total
        invs[qb] = jnp.broadcast_to(norm, (8, width))
        by_row = jnp.transpose(jnp.broadcast_to(norm, (D, width)))
        scaled = (stack_heads(do_ref, qb).astype(F32) * by_row).astype(BF16)
        dop[qb] = scaled
        dvp[qb, pl.ds(0, SLOTS)] = nn(wb[qb], scaled).reshape(SLOTS, BT, D)
        return carry

    lax.fori_loop(0, nq, probs_step, 0)

    def block_sum(part, w):
        acc = None
        for qb in range(nq):
            one = part[qb, table[qb, 2 * SLOTS + w]]
            acc = one if acc is None else acc + one
        return acc

    back = (behind, ahead)
    sets = (
        (dkp, scale, k_send1, k_recv1, k_send2, k_recv2, fin_k),
        (dvp, 1.0, v_send1, v_recv1, v_send2, v_recv2, fin_v),
    )

    def red(a, hop, d, c):
        src, dst = (sets[a][2], sets[a][3]) if hop == 0 else (sets[a][4], sets[a][5])
        return remote(
            src.at[d, c], dst.at[d, c],
            red_ss.at[a, hop, d, c], red_rs.at[a, hop, d, c], {"ctx": back[d]},
        )

    def red_first(a):
        part, factor, send1 = sets[a][:3]
        for c, d in both:
            for b in range(cb):
                w = far[d] * nq + c * cb + b
                send1[d, c, pl.ds(b * BT, BT), :] = (block_sum(part, w) * factor).astype(BF16)
            red(a, 0, d, c).start()

    def red_second(a, c):
        part, factor, _, recv1, send2 = sets[a][:5]
        for d in range(2):
            red(a, 0, d, c).wait_recv()
            for b in range(cb):
                w = near[d] * nq + c * cb + b
                came = recv1[d, c, pl.ds(b * BT, BT), :].astype(F32)
                send2[d, c, pl.ds(b * BT, BT), :] = (block_sum(part, w) * factor + came).astype(BF16)
            red(a, 1, d, c).start()

    def red_last(a):
        part, factor, _, _, _, recv2, fin = sets[a]
        for c in range(CHUNKS):
            for d in range(2):
                red(a, 1, d, c).wait_recv()
            for b in range(cb):
                r = pl.ds(b * BT, BT)
                own = block_sum(part, REACH * nq + c * cb + b) * factor
                whole = own + recv2[0, c, r, :].astype(F32) + recv2[1, c, r, :].astype(F32)
                fin[pl.ds(c * chunk + b * BT, BT), :] = whole.astype(BF16)

    ex_bufs = ((dq_buf, dq_land, dq_out), (fin_k, dk_land, dk_out), (fin_v, dv_land, dv_out))

    def exchange(a, t):
        src, land, _ = ex_bufs[a]
        dev = lax.rem(h + t, n_head)
        return remote(
            src.at[pl.ds(pl.multiple_of(dev * rows, rows), rows), :], land.at[h],
            ex_ss.at[a, t], ex_rs.at[a, t], {"head": dev},
        )

    def exchange_start(a):
        src, land, _ = ex_bufs[a]
        for t in range(1, n_head):
            exchange(a, t).start()
        land[h] = src[pl.ds(pl.multiple_of(h * rows, rows), rows), :]

    def exchange_end(a):
        _, land, out = ex_bufs[a]
        w = land.shape[2]
        for t in range(1, n_head):
            exchange(a, t).wait_recv()
        for j in range(n_head):
            out[:, j * w:(j + 1) * w] = land[j]

    red_first(1)
    for c, d in both:
        win(1, 1, d, c).wait_recv()

    def scores_step(qb, carry):
        for c in range(CHUNKS):
            @pl.when(qb == nq - CHUNKS + c)
            def _():
                red_second(1, c)
        gather_blocks(v_win, SLOTS, qb)
        st[...] = nt(kg[...], dop[qb])
        delta = jnp.zeros((1, width), F32)
        for s in range(SLOTS):
            r = pl.ds(s * BT, BT)
            delta = delta + jnp.sum(wb[qb, r, :].astype(F32) * st[r, :], axis=0, keepdims=True)
        delta = delta * invs[qb, 0:1, :]
        for s in range(SLOTS):
            r = pl.ds(s * BT, BT)
            wb[qb, r, :] = (wb[qb, r, :].astype(F32) * (st[r, :] - delta)).astype(BF16)
        dkp[qb, pl.ds(0, SLOTS)] = nn(wb[qb], stack_heads(q_ref, qb)).reshape(SLOTS, BT, D)
        return carry

    lax.fori_loop(0, nq, scores_step, 0)
    red_first(0)

    def queries_step(qb, carry):
        gather_blocks(k_win, SLOTS, qb)
        dq = (tn(wb[qb], kg[...]) * scale).astype(BF16)
        r = pl.ds(pl.multiple_of(qb * BT, BT), BT)
        for g in range(group):
            dq_buf[r, g * D:(g + 1) * D] = dq[g * BT:(g + 1) * BT, :]
        return carry

    lax.fori_loop(0, nq, queries_step, 0)
    exchange_start(0)
    red_last(1)
    exchange_start(2)
    for c in range(CHUNKS):
        red_second(0, c)
    exchange_end(2)
    red_last(0)
    exchange_start(1)
    exchange_end(0)
    exchange_end(1)

    for c, d in both:
        for a in range(2):
            for hop in range(2):
                win(a, hop, d, c).wait_send()
                red(a, hop, d, c).wait_send()
    for a in range(3):
        for t in range(1, n_head):
            exchange(a, t).wait_send()


def slot_tables(n_ctx, nq, nw, blocks, counts):
    first = (lax.axis_index("ctx") - REACH) * nq
    local = jnp.mod(blocks - first, n_ctx * nq)
    slots = jnp.arange(SLOTS, dtype=jnp.int32)
    live = slots[None] < counts[:, None]
    scored = jnp.where(live, local, local[:, :1])
    zeroed = jnp.where(live, local, nw)
    hit = zeroed[:, None, :] == jnp.arange(nw, dtype=jnp.int32)[None, :, None]
    slot = jnp.min(jnp.where(hit, slots[None, None], SLOTS), axis=2)
    return jnp.concatenate([scored, zeroed, slot], axis=1), live.astype(F32)


def on_device(n_ctx, n_head, queries, keys, values, output_gradient, blocks, counts):
    tok, qw = queries.shape
    group = qw // D
    nq = tok // BT
    nw = SEGS * nq
    rows = tok // n_head
    chunk = tok // CHUNKS
    vmem = pl.BlockSpec(memory_space=pltpu.VMEM)
    smem = pl.BlockSpec(memory_space=pltpu.SMEM)
    hop = pltpu.VMEM((2, CHUNKS, chunk, D), BF16)
    sems = pltpu.SemaphoreType.DMA((2, 2, 2, CHUNKS))
    width = group * BT
    return pl.pallas_call(
        functools.partial(kernel, n_ctx, n_head, tok, group),
        out_shape=(
            jax.ShapeDtypeStruct((rows, n_head * qw), BF16),
            jax.ShapeDtypeStruct((rows, n_head * D), BF16),
            jax.ShapeDtypeStruct((rows, n_head * D), BF16),
        ),
        in_specs=[vmem] * 4 + [smem] * 2,
        out_specs=(vmem,) * 3,
        scratch_shapes=[
            pltpu.VMEM((nw + 1, BT, D), BF16),
            pltpu.VMEM((nw + 1, BT, D), BF16),
            pltpu.VMEM((SLOTS * BT, D), BF16),
            pltpu.VMEM((SLOTS * BT, width), F32),
            pltpu.VMEM((nq, SLOTS * BT, width), BF16),
            pltpu.VMEM((nq, width, D), BF16),
            pltpu.VMEM((nq, 8, width), F32),
            pltpu.VMEM((nq, SLOTS + 1, BT, D), F32),
            pltpu.VMEM((nq, SLOTS + 1, BT, D), F32),
            pltpu.VMEM((tok, qw), BF16),
            hop, hop, hop, hop, hop, hop, hop, hop,
            pltpu.VMEM((tok, D), BF16),
            pltpu.VMEM((tok, D), BF16),
            pltpu.VMEM((n_head, rows, qw), BF16),
            pltpu.VMEM((n_head, rows, D), BF16),
            pltpu.VMEM((n_head, rows, D), BF16),
            sems, sems, sems, sems,
            pltpu.SemaphoreType.DMA((3, n_head)),
            pltpu.SemaphoreType.DMA((3, n_head)),
        ],
        compiler_params=pltpu.CompilerParams(
            collective_id=0, has_side_effects=True, vmem_limit_bytes=60 * 1024 * 1024
        ),
    )(
        queries, keys.reshape(nq, BT, D), values.reshape(nq, BT, D), output_gradient,
        *slot_tables(n_ctx, nq, nw, blocks, counts),
    )


def solution(mesh):
    return jax.shard_map(
        functools.partial(on_device, mesh.shape["ctx"], mesh.shape["head"]),
        mesh=mesh,
        in_specs=(
            P("ctx", "head"),
            P("ctx", "head"),
            P("ctx", "head"),
            P("ctx", "head"),
            P("ctx", None),
            P("ctx"),
        ),
        out_specs=(P(("ctx", "head"), None), P(("ctx", "head"), None), P(("ctx", "head"), None)),
        check_vma=False,
    )
```

```python
import functools
import math

import jax
import jax.numpy as jnp
from jax import lax
from jax.experimental import pallas as pl
from jax.experimental.pallas import tpu as pltpu
from jax.sharding import PartitionSpec as P

D = 128
BT = 128
SLOTS = 8
REACH = 2
SEGS = 2 * REACH + 1
CHUNKS = 2
MESH = pl.DeviceIdType.MESH
F32 = jnp.float32
BF16 = jnp.bfloat16


def nt(a, b):
    return lax.dot_general(a, b, (((1,), (1,)), ((), ())), preferred_element_type=F32)


def nn(a, b):
    return lax.dot_general(a, b, (((1,), (0,)), ((), ())), preferred_element_type=F32)


def tn(a, b):
    return lax.dot_general(a, b, (((0,), (0,)), ((), ())), preferred_element_type=F32)


def slot_table(first, total_blocks, nq, nw, blocks, counts_ref):
    shape = (nq, BT)
    column = lax.broadcasted_iota(jnp.int32, shape, 1)
    row = lax.broadcasted_iota(jnp.int32, shape, 0)
    counts = jnp.zeros(shape, jnp.int32)
    for qb in range(nq):
        counts = jnp.where(row == qb, counts_ref[qb], counts)
    local = blocks - first
    local = jnp.where(local < 0, local + total_blocks, local)
    local = jnp.where(local >= total_blocks, local - total_blocks, local)
    local = jnp.clip(local, 0, nw - 1)
    window_block = column - 2 * SLOTS
    inside = (window_block >= 0) & (window_block < nw)
    table = jnp.where(inside, SLOTS, 0)
    lead = jnp.broadcast_to(local[:, :1], shape)
    for s in range(SLOTS):
        block = jnp.broadcast_to(local[:, s:s + 1], shape)
        live = counts > s
        zeroed = jnp.where(live, block, nw)
        table = jnp.where(column == s, jnp.where(live, block, lead), table)
        table = jnp.where(column == SLOTS + s, zeroed, table)
        table = jnp.where(inside & (window_block == zeroed), s, table)
        table = jnp.where(window_block == nw + s, jnp.where(live, 1, 0), table)
    return table


def kernel(
    n_ctx, n_head, tok, group,
    q_hbm, k_ref, v_ref, do_hbm, blocks_ref, counts_ref,
    dq_land, dk_land, dv_land,
    q_ref, do_ref, mask, table_v, table,
    k_win, v_win, kg, st, wb, dop, invs, dvp, dkp, dq_buf,
    v_send1, v_recv1, v_send2, v_recv2, k_send1, k_recv1, k_send2, k_recv2,
    fin_v, fin_k,
    win_ss, win_rs, red_ss, red_rs, ex_ss, ex_rs, own_s,
):
    nq = tok // BT
    nw = SEGS * nq
    rows = tok // n_head
    chunk = tok // CHUNKS
    cb = chunk // BT
    me = lax.axis_index("ctx")
    h = lax.axis_index("head")
    ahead = lax.rem(me + 1, n_ctx)
    behind = lax.rem(me + n_ctx - 1, n_ctx)
    to = (ahead, behind)
    scale = 1.0 / math.sqrt(D)
    c2 = scale * math.log2(math.e)

    def remote(src, dst, ss, rs, dev):
        return pltpu.make_async_remote_copy(
            src_ref=src, dst_ref=dst, send_sem=ss, recv_sem=rs, device_id=dev, device_id_type=MESH
        )

    loads = [
        pltpu.make_async_copy(k_ref, k_win.at[pl.ds(REACH * nq, nq)], own_s.at[0]),
        pltpu.make_async_copy(q_hbm, q_ref, own_s.at[1]),
        pltpu.make_async_copy(do_hbm, do_ref, own_s.at[2]),
        pltpu.make_async_copy(v_ref, v_win.at[pl.ds(REACH * nq, nq)], own_s.at[3]),
    ]

    barrier = pltpu.get_barrier_semaphore()
    for d in range(2):
        pl.semaphore_signal(barrier, inc=1, device_id={"ctx": to[d]}, device_id_type=MESH)
    for t in range(1, n_head):
        pl.semaphore_signal(
            barrier, inc=1, device_id={"head": lax.rem(h + t, n_head)}, device_id_type=MESH
        )
    pl.semaphore_wait(barrier, 2 + n_head - 1)

    near, far = (1, 3), (0, 4)

    def win(a, hop, d, c):
        ref, window = ((k_ref, k_win), (v_ref, v_win))[a]
        if hop == 0:
            src = ref.at[pl.ds(c * cb, cb)]
            seg = near[d]
        else:
            src = window.at[pl.ds(near[d] * nq + c * cb, cb)]
            seg = far[d]
        dst = window.at[pl.ds(seg * nq + c * cb, cb)]
        return remote(src, dst, win_ss.at[a, hop, d, c], win_rs.at[a, hop, d, c], {"ctx": to[d]})

    both = [(c, d) for c in range(CHUNKS) for d in range(2)]
    for c, d in both:
        win(0, 0, d, c).start()
    for load in loads:
        load.start()

    table_v[pl.ds(0, nq), :] = slot_table(
        (me - REACH) * nq, n_ctx * nq, nq, nw, blocks_ref[...], counts_ref
    )
    table_v[pl.ds(nq, 8 - nq), :] = jnp.zeros((8 - nq, BT), jnp.int32)
    tables = pltpu.make_async_copy(table_v, table, own_s.at[7])
    tables.start()
    mask[0] = jnp.zeros((8, group * BT), F32)
    mask[1] = jnp.ones((8, group * BT), F32)
    k_win[nw] = jnp.zeros((BT, D), BF16)
    v_win[nw] = jnp.zeros((BT, D), BF16)
    for qb in range(nq):
        dvp[qb, SLOTS] = jnp.zeros((BT, D), F32)
        dkp[qb, SLOTS] = jnp.zeros((BT, D), F32)

    for c, d in both:
        win(0, 0, d, c).wait_recv()
        win(0, 1, d, c).start()
    for c, d in both:
        win(1, 0, d, c).start()
    for load in loads:
        load.wait()
    tables.wait()
    for c, d in both:
        win(0, 1, d, c).wait_recv()

    def stack_heads(ref, qb):
        r = pl.ds(pl.multiple_of(qb * BT, BT), BT)
        return jnp.concatenate([ref[r, g * D:(g + 1) * D] for g in range(group)], axis=0)

    def gather_blocks(window, first, qb):
        for s in range(SLOTS):
            kg[pl.ds(s * BT, BT), :] = window[table[qb, first + s]]

    width = group * BT

    def probs_step(qb, carry):
        for c in range(CHUNKS):
            @pl.when(qb == c + 1)
            def _():
                for d in range(2):
                    win(1, 0, d, c).wait_recv()
                    win(1, 1, d, c).start()
        qs = stack_heads(q_ref, qb)
        gather_blocks(k_win, 0, qb)
        st[...] = nt(kg[...], qs)
        top = jnp.max(st[...], axis=0, keepdims=True) * c2
        total = jnp.zeros((8, width), F32)
        for s in range(SLOTS):
            w = jnp.exp2(st[pl.ds(s * BT, BT), :] * c2 - top).astype(BF16)
            part = jnp.sum(w.astype(F32).reshape(-1, 8, width), axis=0)
            total = total + part * mask[table[qb, 2 * SLOTS + nw + s]]
            wb[qb, pl.ds(s * BT, BT), :] = w
        norm = 1.0 / jnp.sum(total, axis=0, keepdims=True)
        invs[qb] = jnp.broadcast_to(norm, (8, width))
        by_row = jnp.transpose(jnp.broadcast_to(norm, (D, width)))
        scaled = (stack_heads(do_ref, qb).astype(F32) * by_row).astype(BF16)
        dop[qb] = scaled
        dvp[qb, pl.ds(0, SLOTS)] = nn(wb[qb], scaled).reshape(SLOTS, BT, D)
        return carry

    lax.fori_loop(0, nq, probs_step, 0)

    def block_sum(part, w):
        acc = None
        for qb in range(nq):
            one = part[qb, table[qb, 2 * SLOTS + w]]
            acc = one if acc is None else acc + one
        return acc

    back = (behind, ahead)
    sets = (
        (dkp, scale, k_send1, k_recv1, k_send2, k_recv2, fin_k),
        (dvp, 1.0, v_send1, v_recv1, v_send2, v_recv2, fin_v),
    )

    def red(a, hop, d, c):
        src, dst = (sets[a][2], sets[a][3]) if hop == 0 else (sets[a][4], sets[a][5])
        return remote(
            src.at[d, c], dst.at[d, c],
            red_ss.at[a, hop, d, c], red_rs.at[a, hop, d, c], {"ctx": back[d]},
        )

    def red_first(a):
        part, factor, send1 = sets[a][:3]
        for c, d in both:
            for b in range(cb):
                w = far[d] * nq + c * cb + b
                send1[d, c, pl.ds(b * BT, BT), :] = (block_sum(part, w) * factor).astype(BF16)
            red(a, 0, d, c).start()

    def red_second(a, c):
        part, factor, _, recv1, send2 = sets[a][:5]
        for d in range(2):
            red(a, 0, d, c).wait_recv()
            for b in range(cb):
                w = near[d] * nq + c * cb + b
                came = recv1[d, c, pl.ds(b * BT, BT), :].astype(F32)
                send2[d, c, pl.ds(b * BT, BT), :] = (block_sum(part, w) * factor + came).astype(BF16)
            red(a, 1, d, c).start()

    def red_last(a):
        part, factor, _, _, _, recv2, fin = sets[a]
        for c in range(CHUNKS):
            for d in range(2):
                red(a, 1, d, c).wait_recv()
            for b in range(cb):
                r = pl.ds(b * BT, BT)
                own = block_sum(part, REACH * nq + c * cb + b) * factor
                whole = own + recv2[0, c, r, :].astype(F32) + recv2[1, c, r, :].astype(F32)
                fin[pl.ds(c * chunk + b * BT, BT), :] = whole.astype(BF16)

    ex_bufs = ((dq_buf, dq_land), (fin_k, dk_land), (fin_v, dv_land))

    def exchange(a, t):
        src, land = ex_bufs[a]
        dev = lax.rem(h + t, n_head)
        return remote(
            src.at[pl.ds(pl.multiple_of(dev * rows, rows), rows), :], land.at[h],
            ex_ss.at[a, t], ex_rs.at[a, t], {"head": dev},
        )

    def own(a):
        src, land = ex_bufs[a]
        mine = src.at[pl.ds(pl.multiple_of(h * rows, rows), rows), :]
        return pltpu.make_async_copy(mine, land.at[h], own_s.at[4 + a])

    def exchange_start(a):
        for t in range(1, n_head):
            exchange(a, t).start()
        own(a).start()

    def exchange_end(a):
        own(a).wait()
        for t in range(1, n_head):
            exchange(a, t).wait_recv()

    red_first(1)
    for c, d in both:
        win(1, 1, d, c).wait_recv()

    def scores_step(qb, carry):
        for c in range(CHUNKS):
            @pl.when(qb == nq - CHUNKS + c)
            def _():
                red_second(1, c)
        gather_blocks(v_win, SLOTS, qb)
        st[...] = nt(kg[...], dop[qb])
        delta = jnp.zeros((1, width), F32)
        for s in range(SLOTS):
            r = pl.ds(s * BT, BT)
            delta = delta + jnp.sum(wb[qb, r, :].astype(F32) * st[r, :], axis=0, keepdims=True)
        delta = delta * invs[qb, 0:1, :]
        for s in range(SLOTS):
            r = pl.ds(s * BT, BT)
            wb[qb, r, :] = (wb[qb, r, :].astype(F32) * (st[r, :] - delta)).astype(BF16)
        dkp[qb, pl.ds(0, SLOTS)] = nn(wb[qb], stack_heads(q_ref, qb)).reshape(SLOTS, BT, D)
        return carry

    lax.fori_loop(0, nq, scores_step, 0)
    red_first(0)

    def queries_step(qb, carry):
        gather_blocks(k_win, SLOTS, qb)
        dq = (tn(wb[qb], kg[...]) * scale).astype(BF16)
        r = pl.ds(pl.multiple_of(qb * BT, BT), BT)
        for g in range(group):
            dq_buf[r, g * D:(g + 1) * D] = dq[g * BT:(g + 1) * BT, :]
        return carry

    lax.fori_loop(0, nq, queries_step, 0)
    exchange_start(0)
    red_last(1)
    exchange_start(2)
    for c in range(CHUNKS):
        red_second(0, c)
    red_last(0)
    exchange_start(1)
    exchange_end(2)
    exchange_end(0)
    exchange_end(1)

    for c, d in both:
        for a in range(2):
            for hop in range(2):
                win(a, hop, d, c).wait_send()
                red(a, hop, d, c).wait_send()
    for a in range(3):
        for t in range(1, n_head):
            exchange(a, t).wait_send()


def assemble(dq_land, dk_land, dv_land, dq_out, dk_out, dv_out):
    for land, out in ((dq_land, dq_out), (dk_land, dk_out), (dv_land, dv_out)):
        parts, _, w = land.shape
        for j in range(parts):
            out[:, j * w:(j + 1) * w] = land[j]


def on_device(n_ctx, n_head, queries, keys, values, output_gradient, blocks, counts):
    tok, qw = queries.shape
    group = qw // D
    nq = tok // BT
    nw = SEGS * nq
    rows = tok // n_head
    chunk = tok // CHUNKS
    vmem = pl.BlockSpec(memory_space=pltpu.VMEM)
    smem = pl.BlockSpec(memory_space=pltpu.SMEM)
    hop = pltpu.VMEM((2, CHUNKS, chunk, D), BF16)
    sems = pltpu.SemaphoreType.DMA((2, 2, 2, CHUNKS))
    width = group * BT
    hbm = pl.BlockSpec(memory_space=pl.ANY)
    landed = pl.pallas_call(
        functools.partial(kernel, n_ctx, n_head, tok, group),
        out_shape=(
            jax.ShapeDtypeStruct((n_head, rows, qw), BF16),
            jax.ShapeDtypeStruct((n_head, rows, D), BF16),
            jax.ShapeDtypeStruct((n_head, rows, D), BF16),
        ),
        in_specs=[hbm] * 4 + [vmem, smem],
        out_specs=(hbm,) * 3,
        scratch_shapes=[
            pltpu.VMEM((tok, qw), BF16),
            pltpu.VMEM((tok, qw), BF16),
            pltpu.VMEM((2, 8, width), F32),
            pltpu.VMEM((8, BT), jnp.int32),
            pltpu.SMEM((8, BT), jnp.int32),
            pltpu.VMEM((nw + 1, BT, D), BF16),
            pltpu.VMEM((nw + 1, BT, D), BF16),
            pltpu.VMEM((SLOTS * BT, D), BF16),
            pltpu.VMEM((SLOTS * BT, width), F32),
            pltpu.VMEM((nq, SLOTS * BT, width), BF16),
            pltpu.VMEM((nq, width, D), BF16),
            pltpu.VMEM((nq, 8, width), F32),
            pltpu.VMEM((nq, SLOTS + 1, BT, D), F32),
            pltpu.VMEM((nq, SLOTS + 1, BT, D), F32),
            pltpu.VMEM((tok, qw), BF16),
            hop, hop, hop, hop, hop, hop, hop, hop,
            pltpu.VMEM((tok, D), BF16),
            pltpu.VMEM((tok, D), BF16),
            sems, sems, sems, sems,
            pltpu.SemaphoreType.DMA((3, n_head)),
            pltpu.SemaphoreType.DMA((3, n_head)),
            pltpu.SemaphoreType.DMA((8,)),
        ],
        compiler_params=pltpu.CompilerParams(
            collective_id=0, has_side_effects=True, vmem_limit_bytes=60 * 1024 * 1024
        ),
    )(
        queries, keys.reshape(nq, BT, D), values.reshape(nq, BT, D), output_gradient, blocks, counts
    )
    return pl.pallas_call(
        assemble,
        out_shape=(
            jax.ShapeDtypeStruct((rows, n_head * qw), BF16),
            jax.ShapeDtypeStruct((rows, n_head * D), BF16),
            jax.ShapeDtypeStruct((rows, n_head * D), BF16),
        ),
        in_specs=[vmem] * 3,
        out_specs=(vmem,) * 3,
    )(*landed)


def solution(mesh):
    return jax.shard_map(
        functools.partial(on_device, mesh.shape["ctx"], mesh.shape["head"]),
        mesh=mesh,
        in_specs=(
            P("ctx", "head"),
            P("ctx", "head"),
            P("ctx", "head"),
            P("ctx", "head"),
            P("ctx", None),
            P("ctx"),
        ),
        out_specs=(P(("ctx", "head"), None), P(("ctx", "head"), None), P(("ctx", "head"), None)),
        check_vma=False,
    )
```

```python
import functools
import math

import jax
import jax.numpy as jnp
from jax import lax
from jax.experimental import pallas as pl
from jax.experimental.pallas import tpu as pltpu
from jax.sharding import PartitionSpec as P

D = 128
BT = 128
SLOTS = 8
REACH = 2
SEGS = 2 * REACH + 1
CHUNKS = 2
UNROLL = 8
MESH = pl.DeviceIdType.MESH
F32 = jnp.float32
BF16 = jnp.bfloat16


def nt(a, b):
    return lax.dot_general(a, b, (((1,), (1,)), ((), ())), preferred_element_type=F32)


def nn(a, b):
    return lax.dot_general(a, b, (((1,), (0,)), ((), ())), preferred_element_type=F32)


def tn(a, b):
    return lax.dot_general(a, b, (((0,), (0,)), ((), ())), preferred_element_type=F32)


def slot_table(first, total_blocks, nq, nw, blocks, counts_ref):
    shape = (nq, BT)
    column = lax.broadcasted_iota(jnp.int32, shape, 1)
    row = lax.broadcasted_iota(jnp.int32, shape, 0)
    counts = jnp.zeros(shape, jnp.int32)
    for qb in range(nq):
        counts = jnp.where(row == qb, counts_ref[qb], counts)
    local = blocks - first
    local = jnp.where(local < 0, local + total_blocks, local)
    local = jnp.where(local >= total_blocks, local - total_blocks, local)
    local = jnp.clip(local, 0, nw - 1)
    window_block = column - 2 * SLOTS
    inside = (window_block >= 0) & (window_block < nw)
    table = jnp.where(inside, SLOTS, 0)
    lead = jnp.broadcast_to(local[:, :1], shape)
    for s in range(SLOTS):
        block = jnp.broadcast_to(local[:, s:s + 1], shape)
        live = counts > s
        zeroed = jnp.where(live, block, nw)
        table = jnp.where(column == s, jnp.where(live, block, lead), table)
        table = jnp.where(column == SLOTS + s, zeroed, table)
        table = jnp.where(inside & (window_block == zeroed), s, table)
        table = jnp.where(window_block == nw + s, jnp.where(live, 1, 0), table)
    return table


def kernel(
    n_ctx, n_head, tok, group,
    q_hbm, k_ref, v_ref, do_hbm, blocks_ref, counts_ref,
    dq_land, dk_land, dv_land,
    q_ref, do_ref, mask, table_v, table,
    k_win, v_win, kg, st, wb, dop, invs, dvp, dkp, dq_buf,
    v_send1, v_recv1, v_send2, v_recv2, k_send1, k_recv1, k_send2, k_recv2,
    fin_v, fin_k,
    win_ss, win_rs, red_ss, red_rs, ex_ss, ex_rs, own_s, head_s,
):
    nq = tok // BT
    nw = SEGS * nq
    width = group * BT
    rows = tok // n_head
    chunk = tok // CHUNKS
    cb = chunk // BT
    me = lax.axis_index("ctx")
    h = lax.axis_index("head")
    ahead = lax.rem(me + 1, n_ctx)
    behind = lax.rem(me + n_ctx - 1, n_ctx)
    to = (ahead, behind)
    scale = 1.0 / math.sqrt(D)
    c2 = scale * math.log2(math.e)

    def remote(src, dst, ss, rs, dev):
        return pltpu.make_async_remote_copy(
            src_ref=src, dst_ref=dst, send_sem=ss, recv_sem=rs, device_id=dev, device_id_type=MESH
        )

    loads = [
        pltpu.make_async_copy(k_ref, k_win.at[pl.ds(REACH * nq, nq)], own_s.at[0]),
        pltpu.make_async_copy(v_ref, v_win.at[pl.ds(REACH * nq, nq)], own_s.at[1]),
    ]
    for g in range(group):
        cols = pl.ds(g * D, D)
        loads.append(pltpu.make_async_copy(q_hbm.at[:, :, cols], q_ref.at[:, g], head_s.at[0, g]))
        loads.append(pltpu.make_async_copy(do_hbm.at[:, :, cols], do_ref.at[:, g], head_s.at[1, g]))

    barrier = pltpu.get_barrier_semaphore()
    for d in range(2):
        pl.semaphore_signal(barrier, inc=1, device_id={"ctx": to[d]}, device_id_type=MESH)
    for t in range(1, n_head):
        pl.semaphore_signal(
            barrier, inc=1, device_id={"head": lax.rem(h + t, n_head)}, device_id_type=MESH
        )
    pl.semaphore_wait(barrier, 2 + n_head - 1)

    near, far = (1, 3), (0, 4)

    def win(a, hop, d, c):
        ref, window = ((k_ref, k_win), (v_ref, v_win))[a]
        if hop == 0:
            src = ref.at[pl.ds(c * cb, cb)]
            seg = near[d]
        else:
            src = window.at[pl.ds(near[d] * nq + c * cb, cb)]
            seg = far[d]
        dst = window.at[pl.ds(seg * nq + c * cb, cb)]
        return remote(src, dst, win_ss.at[a, hop, d, c], win_rs.at[a, hop, d, c], {"ctx": to[d]})

    both = [(c, d) for c in range(CHUNKS) for d in range(2)]
    for c, d in both:
        win(0, 0, d, c).start()
    for load in loads:
        load.start()

    table_v[pl.ds(0, nq), :] = slot_table(
        (me - REACH) * nq, n_ctx * nq, nq, nw, blocks_ref[...], counts_ref
    )
    table_v[pl.ds(nq, 8 - nq), :] = jnp.zeros((8 - nq, BT), jnp.int32)
    tables = pltpu.make_async_copy(table_v, table, own_s.at[7])
    tables.start()
    mask[0] = jnp.zeros((8, group * BT), F32)
    mask[1] = jnp.ones((8, group * BT), F32)
    k_win[nw] = jnp.zeros((BT, D), BF16)
    v_win[nw] = jnp.zeros((BT, D), BF16)
    for qb in range(nq):
        dvp[qb, SLOTS] = jnp.zeros((BT, D), F32)
        dkp[qb, SLOTS] = jnp.zeros((BT, D), F32)

    for c, d in both:
        win(0, 0, d, c).wait_recv()
        win(0, 1, d, c).start()
    for c, d in both:
        win(1, 0, d, c).start()
    for load in loads:
        load.wait()
    tables.wait()
    for c, d in both:
        win(0, 1, d, c).wait_recv()

    def stacked(ref, qb):
        return ref[qb].reshape(width, D)

    def fold(x):
        return x.reshape(-1, 8, width)

    def gather_blocks(window, first, qb):
        for s in range(SLOTS):
            kg[pl.ds(s * BT, BT), :] = window[table[qb, first + s]]

    top = None
    for t in range(nq + 2):
        for c in range(CHUNKS):
            if t == 2 * c + 3:
                for d in range(2):
                    win(1, 0, d, c).wait_recv()
                    win(1, 1, d, c).start()

        def probs_step(i, carry, t=t, top=top):
            tops, total = carry
            group_of = pl.ds(i * UNROLL, UNROLL)
            if t < nq:
                blocks = [k_win[table[t, i * UNROLL + u]] for u in range(UNROLL)]
                tile = nt(jnp.concatenate(blocks, axis=0), stacked(q_ref, t))
                st[t % 2, group_of] = tile.reshape(UNROLL, BT, width)
                tops = jnp.maximum(tops, jnp.max(fold(tile), axis=0))
            if 1 <= t <= nq:
                for u in range(UNROLL):
                    s = i * UNROLL + u
                    w = jnp.exp2(fold(st[(t - 1) % 2, s]) * c2 - top[None])
                    w = w.reshape(BT, width).astype(BF16)
                    alive = mask[table[t - 1, 2 * SLOTS + nw + s]]
                    total = total + jnp.sum(fold(w.astype(F32)), axis=0) * alive
                    wb[t - 1, s] = w
            if t >= 2:
                tile = nn(wb[t - 2, group_of].reshape(UNROLL * BT, width), dop[t - 2])
                dvp[t - 2, group_of] = tile.reshape(UNROLL, BT, D)
            return tops, total

        start = (jnp.full((8, width), -jnp.inf, F32), jnp.zeros((8, width), F32))
        tops, total = lax.fori_loop(0, SLOTS // UNROLL, probs_step, start)
        if t < nq:
            top = jnp.broadcast_to(jnp.max(tops, axis=0, keepdims=True) * c2, (8, width))
        if 1 <= t <= nq:
            norm = 1.0 / jnp.sum(total, axis=0, keepdims=True)
            invs[t - 1] = jnp.broadcast_to(norm, (8, width))
            by_row = jnp.transpose(jnp.broadcast_to(norm, (D, width)))
            dop[t - 1] = (stacked(do_ref, t - 1).astype(F32) * by_row).astype(BF16)

    def block_sum(part, w):
        acc = None
        for qb in range(nq):
            one = part[qb, table[qb, 2 * SLOTS + w]]
            acc = one if acc is None else acc + one
        return acc

    back = (behind, ahead)
    sets = (
        (dkp, scale, k_send1, k_recv1, k_send2, k_recv2, fin_k),
        (dvp, 1.0, v_send1, v_recv1, v_send2, v_recv2, fin_v),
    )

    def red(a, hop, d, c):
        src, dst = (sets[a][2], sets[a][3]) if hop == 0 else (sets[a][4], sets[a][5])
        return remote(
            src.at[d, c], dst.at[d, c],
            red_ss.at[a, hop, d, c], red_rs.at[a, hop, d, c], {"ctx": back[d]},
        )

    def red_first(a):
        part, factor, send1 = sets[a][:3]
        for c, d in both:
            for b in range(cb):
                w = far[d] * nq + c * cb + b
                send1[d, c, pl.ds(b * BT, BT), :] = (block_sum(part, w) * factor).astype(BF16)
            red(a, 0, d, c).start()

    def red_second(a, c):
        part, factor, _, recv1, send2 = sets[a][:5]
        for d in range(2):
            red(a, 0, d, c).wait_recv()
            for b in range(cb):
                w = near[d] * nq + c * cb + b
                came = recv1[d, c, pl.ds(b * BT, BT), :].astype(F32)
                send2[d, c, pl.ds(b * BT, BT), :] = (block_sum(part, w) * factor + came).astype(BF16)
            red(a, 1, d, c).start()

    def red_last(a):
        part, factor, _, _, _, recv2, fin = sets[a]
        for c in range(CHUNKS):
            for d in range(2):
                red(a, 1, d, c).wait_recv()
            for b in range(cb):
                r = pl.ds(b * BT, BT)
                own = block_sum(part, REACH * nq + c * cb + b) * factor
                whole = own + recv2[0, c, r, :].astype(F32) + recv2[1, c, r, :].astype(F32)
                fin[pl.ds(c * chunk + b * BT, BT), :] = whole.astype(BF16)

    ex_bufs = ((dq_buf, dq_land), (fin_k, dk_land), (fin_v, dv_land))

    def exchange(a, t):
        src, land = ex_bufs[a]
        dev = lax.rem(h + t, n_head)
        return remote(
            src.at[pl.ds(pl.multiple_of(dev * rows, rows), rows), :], land.at[h],
            ex_ss.at[a, t], ex_rs.at[a, t], {"head": dev},
        )

    def own(a):
        src, land = ex_bufs[a]
        mine = src.at[pl.ds(pl.multiple_of(h * rows, rows), rows), :]
        return pltpu.make_async_copy(mine, land.at[h], own_s.at[4 + a])

    def exchange_start(a):
        for t in range(1, n_head):
            exchange(a, t).start()
        own(a).start()

    def exchange_end(a):
        own(a).wait()
        for t in range(1, n_head):
            exchange(a, t).wait_recv()

    red_first(1)
    for c, d in both:
        win(1, 1, d, c).wait_recv()

    shift = None
    for t in range(nq + 2):
        for c in range(CHUNKS):
            if t == 2 * c + 3:
                red_second(1, c)

        def scores_step(i, delta, t=t, shift=shift):
            group_of = pl.ds(i * UNROLL, UNROLL)
            if t < nq:
                blocks = [v_win[table[t, SLOTS + i * UNROLL + u]] for u in range(UNROLL)]
                tile = nt(jnp.concatenate(blocks, axis=0), dop[t])
                st[t % 2, group_of] = tile.reshape(UNROLL, BT, width)
                weights = wb[t, group_of].reshape(UNROLL * BT, width)
                delta = delta + jnp.sum(fold(weights.astype(F32) * tile), axis=0)
            if 1 <= t <= nq:
                for u in range(UNROLL):
                    s = i * UNROLL + u
                    centred = fold(st[(t - 1) % 2, s]) - shift[None]
                    ds = fold(wb[t - 1, s].astype(F32)) * centred
                    wb[t - 1, s] = ds.reshape(BT, width).astype(BF16)
            if t >= 2:
                tile = nn(wb[t - 2, group_of].reshape(UNROLL * BT, width), stacked(q_ref, t - 2))
                dkp[t - 2, group_of] = tile.reshape(UNROLL, BT, D)
            return delta

        delta = lax.fori_loop(0, SLOTS // UNROLL, scores_step, jnp.zeros((8, width), F32))
        if t < nq:
            whole = jnp.sum(delta, axis=0, keepdims=True) * invs[t, 0:1, :]
            shift = jnp.broadcast_to(whole, (8, width))

    red_first(0)

    def queries_step(qb, carry):
        gather_blocks(k_win, SLOTS, qb)
        dq = (tn(wb[qb].reshape(SLOTS * BT, width), kg[...]) * scale).astype(BF16)
        r = pl.ds(pl.multiple_of(qb * BT, BT), BT)
        for g in range(group):
            dq_buf[r, g * D:(g + 1) * D] = dq[g * BT:(g + 1) * BT, :]
        return carry

    lax.fori_loop(0, nq, queries_step, 0)
    exchange_start(0)
    red_last(1)
    exchange_start(2)
    for c in range(CHUNKS):
        red_second(0, c)
    red_last(0)
    exchange_start(1)
    exchange_end(2)
    exchange_end(0)
    exchange_end(1)

    for c, d in both:
        for a in range(2):
            for hop in range(2):
                win(a, hop, d, c).wait_send()
                red(a, hop, d, c).wait_send()
    for a in range(3):
        for t in range(1, n_head):
            exchange(a, t).wait_send()


def assemble(dq_land, dk_land, dv_land, dq_out, dk_out, dv_out):
    for land, out in ((dq_land, dq_out), (dk_land, dk_out), (dv_land, dv_out)):
        parts, _, w = land.shape
        for j in range(parts):
            out[:, j * w:(j + 1) * w] = land[j]


def on_device(n_ctx, n_head, queries, keys, values, output_gradient, blocks, counts):
    tok, qw = queries.shape
    group = qw // D
    nq = tok // BT
    nw = SEGS * nq
    rows = tok // n_head
    chunk = tok // CHUNKS
    vmem = pl.BlockSpec(memory_space=pltpu.VMEM)
    smem = pl.BlockSpec(memory_space=pltpu.SMEM)
    hop = pltpu.VMEM((2, CHUNKS, chunk, D), BF16)
    sems = pltpu.SemaphoreType.DMA((2, 2, 2, CHUNKS))
    width = group * BT
    hbm = pl.BlockSpec(memory_space=pl.ANY)
    landed = pl.pallas_call(
        functools.partial(kernel, n_ctx, n_head, tok, group),
        out_shape=(
            jax.ShapeDtypeStruct((n_head, rows, qw), BF16),
            jax.ShapeDtypeStruct((n_head, rows, D), BF16),
            jax.ShapeDtypeStruct((n_head, rows, D), BF16),
        ),
        in_specs=[hbm] * 4 + [vmem, smem],
        out_specs=(hbm,) * 3,
        scratch_shapes=[
            pltpu.VMEM((nq, group, BT, D), BF16),
            pltpu.VMEM((nq, group, BT, D), BF16),
            pltpu.VMEM((2, 8, width), F32),
            pltpu.VMEM((8, BT), jnp.int32),
            pltpu.SMEM((8, BT), jnp.int32),
            pltpu.VMEM((nw + 1, BT, D), BF16),
            pltpu.VMEM((nw + 1, BT, D), BF16),
            pltpu.VMEM((SLOTS * BT, D), BF16),
            pltpu.VMEM((2, SLOTS, BT, width), F32),
            pltpu.VMEM((nq, SLOTS, BT, width), BF16),
            pltpu.VMEM((nq, width, D), BF16),
            pltpu.VMEM((nq, 8, width), F32),
            pltpu.VMEM((nq, SLOTS + 1, BT, D), F32),
            pltpu.VMEM((nq, SLOTS + 1, BT, D), F32),
            pltpu.VMEM((tok, qw), BF16),
            hop, hop, hop, hop, hop, hop, hop, hop,
            pltpu.VMEM((tok, D), BF16),
            pltpu.VMEM((tok, D), BF16),
            sems, sems, sems, sems,
            pltpu.SemaphoreType.DMA((3, n_head)),
            pltpu.SemaphoreType.DMA((3, n_head)),
            pltpu.SemaphoreType.DMA((8,)),
            pltpu.SemaphoreType.DMA((2, group)),
        ],
        compiler_params=pltpu.CompilerParams(
            collective_id=0, has_side_effects=True, vmem_limit_bytes=60 * 1024 * 1024
        ),
    )(
        queries.reshape(nq, BT, qw), keys.reshape(nq, BT, D), values.reshape(nq, BT, D),
        output_gradient.reshape(nq, BT, qw), blocks, counts,
    )
    return pl.pallas_call(
        assemble,
        out_shape=(
            jax.ShapeDtypeStruct((rows, n_head * qw), BF16),
            jax.ShapeDtypeStruct((rows, n_head * D), BF16),
            jax.ShapeDtypeStruct((rows, n_head * D), BF16),
        ),
        in_specs=[vmem] * 3,
        out_specs=(vmem,) * 3,
    )(*landed)


def solution(mesh):
    return jax.shard_map(
        functools.partial(on_device, mesh.shape["ctx"], mesh.shape["head"]),
        mesh=mesh,
        in_specs=(
            P("ctx", "head"),
            P("ctx", "head"),
            P("ctx", "head"),
            P("ctx", "head"),
            P("ctx", None),
            P("ctx"),
        ),
        out_specs=(P(("ctx", "head"), None), P(("ctx", "head"), None), P(("ctx", "head"), None)),
        check_vma=False,
    )
```

```python
import functools
import math

import jax
import jax.numpy as jnp
from jax import lax
from jax.experimental import pallas as pl
from jax.experimental.pallas import tpu as pltpu
from jax.sharding import PartitionSpec as P

D = 128
BT = 128
SLOTS = 8
REACH = 2
SEGS = 2 * REACH + 1
CHUNKS = 2
UNROLL = 8
MESH = pl.DeviceIdType.MESH
F32 = jnp.float32
BF16 = jnp.bfloat16


def nt(a, b):
    return lax.dot_general(a, b, (((1,), (1,)), ((), ())), preferred_element_type=F32)


def nn(a, b):
    return lax.dot_general(a, b, (((1,), (0,)), ((), ())), preferred_element_type=F32)


def tn(a, b):
    return lax.dot_general(a, b, (((0,), (0,)), ((), ())), preferred_element_type=F32)


def slot_table(first, total_blocks, nq, nw, blocks, counts_ref):
    shape = (nq, BT)
    column = lax.broadcasted_iota(jnp.int32, shape, 1)
    row = lax.broadcasted_iota(jnp.int32, shape, 0)
    counts = jnp.zeros(shape, jnp.int32)
    for qb in range(nq):
        counts = jnp.where(row == qb, counts_ref[qb], counts)
    local = blocks - first
    local = jnp.where(local < 0, local + total_blocks, local)
    local = jnp.where(local >= total_blocks, local - total_blocks, local)
    local = jnp.clip(local, 0, nw - 1)
    window_block = column - 2 * SLOTS
    inside = (window_block >= 0) & (window_block < nw)
    table = jnp.where(inside, SLOTS, 0)
    lead = jnp.broadcast_to(local[:, :1], shape)
    for s in range(SLOTS):
        block = jnp.broadcast_to(local[:, s:s + 1], shape)
        live = counts > s
        zeroed = jnp.where(live, block, nw)
        table = jnp.where(column == s, jnp.where(live, block, lead), table)
        table = jnp.where(column == SLOTS + s, zeroed, table)
        table = jnp.where(inside & (window_block == zeroed), s, table)
        table = jnp.where(window_block == nw + s, jnp.where(live, 1, 0), table)
    return table


def kernel(
    n_ctx, n_head, tok, group,
    q_hbm, k_ref, v_ref, do_hbm, blocks_ref, counts_ref,
    dq_land, dk_land, dv_land,
    q_ref, do_ref, mask, table_v, table,
    k_win, v_win, st, wb, dop, invs, dvp, dkp, dq_buf,
    v_send1, v_recv1, v_send2, v_recv2, k_send1, k_recv1, k_send2, k_recv2,
    fin_v, fin_k,
    win_ss, win_rs, red_ss, red_rs, ex_ss, ex_rs, own_s, head_s,
):
    nq = tok // BT
    nw = SEGS * nq
    width = group * BT
    rows = tok // n_head
    chunk = tok // CHUNKS
    cb = chunk // BT
    me = lax.axis_index("ctx")
    h = lax.axis_index("head")
    ahead = lax.rem(me + 1, n_ctx)
    behind = lax.rem(me + n_ctx - 1, n_ctx)
    to = (ahead, behind)
    scale = 1.0 / math.sqrt(D)
    c2 = scale * math.log2(math.e)

    def remote(src, dst, ss, rs, dev):
        return pltpu.make_async_remote_copy(
            src_ref=src, dst_ref=dst, send_sem=ss, recv_sem=rs, device_id=dev, device_id_type=MESH
        )

    loads = [
        pltpu.make_async_copy(k_ref, k_win.at[pl.ds(REACH * nq, nq)], own_s.at[0]),
        pltpu.make_async_copy(v_ref, v_win.at[pl.ds(REACH * nq, nq)], own_s.at[1]),
    ]
    for g in range(group):
        cols = pl.ds(g * D, D)
        loads.append(pltpu.make_async_copy(q_hbm.at[:, :, cols], q_ref.at[:, g], head_s.at[0, g]))
        loads.append(pltpu.make_async_copy(do_hbm.at[:, :, cols], do_ref.at[:, g], head_s.at[1, g]))

    barrier = pltpu.get_barrier_semaphore()
    for d in range(2):
        pl.semaphore_signal(barrier, inc=1, device_id={"ctx": to[d]}, device_id_type=MESH)
    for t in range(1, n_head):
        pl.semaphore_signal(
            barrier, inc=1, device_id={"head": lax.rem(h + t, n_head)}, device_id_type=MESH
        )
    pl.semaphore_wait(barrier, 2 + n_head - 1)

    near, far = (1, 3), (0, 4)

    def win(a, hop, d, c):
        ref, window = ((k_ref, k_win), (v_ref, v_win))[a]
        if hop == 0:
            src = ref.at[pl.ds(c * cb, cb)]
            seg = near[d]
        else:
            src = window.at[pl.ds(near[d] * nq + c * cb, cb)]
            seg = far[d]
        dst = window.at[pl.ds(seg * nq + c * cb, cb)]
        return remote(src, dst, win_ss.at[a, hop, d, c], win_rs.at[a, hop, d, c], {"ctx": to[d]})

    both = [(c, d) for c in range(CHUNKS) for d in range(2)]
    for c, d in both:
        win(0, 0, d, c).start()
    for load in loads:
        load.start()

    table_v[pl.ds(0, nq), :] = slot_table(
        (me - REACH) * nq, n_ctx * nq, nq, nw, blocks_ref[...], counts_ref
    )
    table_v[pl.ds(nq, 8 - nq), :] = jnp.zeros((8 - nq, BT), jnp.int32)
    tables = pltpu.make_async_copy(table_v, table, own_s.at[7])
    tables.start()
    mask[0] = jnp.zeros((8, group * BT), F32)
    mask[1] = jnp.ones((8, group * BT), F32)
    k_win[nw] = jnp.zeros((BT, D), BF16)
    v_win[nw] = jnp.zeros((BT, D), BF16)
    for qb in range(nq):
        dvp[qb, SLOTS] = jnp.zeros((BT, D), F32)
        dkp[qb, SLOTS] = jnp.zeros((BT, D), F32)

    for c, d in both:
        win(0, 0, d, c).wait_recv()
        win(0, 1, d, c).start()
    for c, d in both:
        win(1, 0, d, c).start()
    for load in loads:
        load.wait()
    tables.wait()
    for c, d in both:
        win(0, 1, d, c).wait_recv()

    def stacked(ref, qb):
        return ref[qb].reshape(width, D)

    def fold(x):
        return x.reshape(-1, 8, width)

    top = None
    for t in range(nq + 2):
        for c in range(CHUNKS):
            if t == 2 * c + 2:
                for d in range(2):
                    win(1, 0, d, c).wait_recv()
                    win(1, 1, d, c).start()

        def probs_step(i, carry, t=t, top=top):
            tops, total = carry
            group_of = pl.ds(i * UNROLL, UNROLL)
            if t < nq:
                blocks = [k_win[table[t, i * UNROLL + u]] for u in range(UNROLL)]
                tile = nt(jnp.concatenate(blocks, axis=0), stacked(q_ref, t))
                st[t % 2, group_of] = tile.reshape(UNROLL, BT, width)
                tops = jnp.maximum(tops, jnp.max(fold(tile), axis=0))
            if 1 <= t <= nq:
                for u in range(UNROLL):
                    s = i * UNROLL + u
                    w = jnp.exp2(fold(st[(t - 1) % 2, s]) * c2 - top[None])
                    w = w.reshape(BT, width).astype(BF16)
                    alive = mask[table[t - 1, 2 * SLOTS + nw + s]]
                    total = total + jnp.sum(fold(w.astype(F32)), axis=0) * alive
                    wb[t - 1, s] = w
            if t >= 2:
                tile = nn(wb[t - 2, group_of].reshape(UNROLL * BT, width), dop[t - 2])
                dvp[t - 2, group_of] = tile.reshape(UNROLL, BT, D)
            return tops, total

        start = (jnp.full((8, width), -jnp.inf, F32), jnp.zeros((8, width), F32))
        tops, total = lax.fori_loop(0, SLOTS // UNROLL, probs_step, start)
        if t < nq:
            top = jnp.broadcast_to(jnp.max(tops, axis=0, keepdims=True) * c2, (8, width))
        if 1 <= t <= nq:
            norm = 1.0 / jnp.sum(total, axis=0, keepdims=True)
            invs[t - 1] = jnp.broadcast_to(norm, (8, width))
            by_row = jnp.transpose(jnp.broadcast_to(norm, (D, width)))
            dop[t - 1] = (stacked(do_ref, t - 1).astype(F32) * by_row).astype(BF16)

    def block_sum(part, w):
        acc = None
        for qb in range(nq):
            one = part[qb, table[qb, 2 * SLOTS + w]]
            acc = one if acc is None else acc + one
        return acc

    back = (behind, ahead)
    sets = (
        (dkp, scale, k_send1, k_recv1, k_send2, k_recv2, fin_k),
        (dvp, 1.0, v_send1, v_recv1, v_send2, v_recv2, fin_v),
    )

    def red(a, hop, d, c):
        src, dst = (sets[a][2], sets[a][3]) if hop == 0 else (sets[a][4], sets[a][5])
        return remote(
            src.at[d, c], dst.at[d, c],
            red_ss.at[a, hop, d, c], red_rs.at[a, hop, d, c], {"ctx": back[d]},
        )

    def red_first(a):
        part, factor, send1 = sets[a][:3]
        for c, d in both:
            for b in range(cb):
                w = far[d] * nq + c * cb + b
                send1[d, c, pl.ds(b * BT, BT), :] = (block_sum(part, w) * factor).astype(BF16)
            red(a, 0, d, c).start()

    def red_second(a, c):
        part, factor, _, recv1, send2 = sets[a][:5]
        for d in range(2):
            red(a, 0, d, c).wait_recv()
            for b in range(cb):
                w = near[d] * nq + c * cb + b
                came = recv1[d, c, pl.ds(b * BT, BT), :].astype(F32)
                send2[d, c, pl.ds(b * BT, BT), :] = (block_sum(part, w) * factor + came).astype(BF16)
            red(a, 1, d, c).start()

    def red_last(a):
        part, factor, _, _, _, recv2, fin = sets[a]
        for c in range(CHUNKS):
            for d in range(2):
                red(a, 1, d, c).wait_recv()
            for b in range(cb):
                r = pl.ds(b * BT, BT)
                own = block_sum(part, REACH * nq + c * cb + b) * factor
                whole = own + recv2[0, c, r, :].astype(F32) + recv2[1, c, r, :].astype(F32)
                fin[pl.ds(c * chunk + b * BT, BT), :] = whole.astype(BF16)

    ex_bufs = ((dq_buf, dq_land), (fin_k, dk_land), (fin_v, dv_land))

    def exchange(a, t):
        src, land = ex_bufs[a]
        dev = lax.rem(h + t, n_head)
        return remote(
            src.at[pl.ds(pl.multiple_of(dev * rows, rows), rows), :], land.at[h],
            ex_ss.at[a, t], ex_rs.at[a, t], {"head": dev},
        )

    def own(a):
        src, land = ex_bufs[a]
        mine = src.at[pl.ds(pl.multiple_of(h * rows, rows), rows), :]
        return pltpu.make_async_copy(mine, land.at[h], own_s.at[4 + a])

    def exchange_start(a):
        for t in range(1, n_head):
            exchange(a, t).start()
        own(a).start()

    def exchange_end(a):
        own(a).wait()
        for t in range(1, n_head):
            exchange(a, t).wait_recv()

    red_first(1)
    for c, d in both:
        win(1, 1, d, c).wait_recv()

    shift = None
    for t in range(nq + 2):
        for c in range(CHUNKS):
            if t == c + 3:
                red_second(1, c)

        def scores_step(i, delta, t=t, shift=shift):
            group_of = pl.ds(i * UNROLL, UNROLL)
            if t < nq:
                blocks = [v_win[table[t, SLOTS + i * UNROLL + u]] for u in range(UNROLL)]
                tile = nt(jnp.concatenate(blocks, axis=0), dop[t])
                st[t % 2, group_of] = tile.reshape(UNROLL, BT, width)
                weights = wb[t, group_of].reshape(UNROLL * BT, width)
                delta = delta + jnp.sum(fold(weights.astype(F32) * tile), axis=0)
            if 1 <= t <= nq:
                for u in range(UNROLL):
                    s = i * UNROLL + u
                    centred = fold(st[(t - 1) % 2, s]) - shift[None]
                    ds = fold(wb[t - 1, s].astype(F32)) * centred
                    wb[t - 1, s] = ds.reshape(BT, width).astype(BF16)
            if t >= 2:
                tile = nn(wb[t - 2, group_of].reshape(UNROLL * BT, width), stacked(q_ref, t - 2))
                dkp[t - 2, group_of] = tile.reshape(UNROLL, BT, D)
                blocks = [k_win[table[t - 2, SLOTS + s]] for s in range(SLOTS)]
                terms = wb[t - 2].reshape(SLOTS * BT, width)
                dq = (tn(terms, jnp.concatenate(blocks, axis=0)) * scale).astype(BF16)
                for g in range(group):
                    rows_of = pl.ds((t - 2) * BT, BT)
                    dq_buf[rows_of, g * D:(g + 1) * D] = dq[g * BT:(g + 1) * BT, :]
            return delta

        delta = lax.fori_loop(0, SLOTS // UNROLL, scores_step, jnp.zeros((8, width), F32))
        if t < nq:
            whole = jnp.sum(delta, axis=0, keepdims=True) * invs[t, 0:1, :]
            shift = jnp.broadcast_to(whole, (8, width))

    exchange_start(0)
    red_first(0)
    red_last(1)
    exchange_start(2)
    for c in range(CHUNKS):
        red_second(0, c)
    red_last(0)
    exchange_start(1)
    exchange_end(2)
    exchange_end(0)
    exchange_end(1)

    for c, d in both:
        for a in range(2):
            for hop in range(2):
                win(a, hop, d, c).wait_send()
                red(a, hop, d, c).wait_send()
    for a in range(3):
        for t in range(1, n_head):
            exchange(a, t).wait_send()


def assemble(dq_land, dk_land, dv_land, dq_out, dk_out, dv_out):
    for land, out in ((dq_land, dq_out), (dk_land, dk_out), (dv_land, dv_out)):
        parts, _, w = land.shape
        for j in range(parts):
            out[:, j * w:(j + 1) * w] = land[j]


def on_device(n_ctx, n_head, queries, keys, values, output_gradient, blocks, counts):
    tok, qw = queries.shape
    group = qw // D
    nq = tok // BT
    nw = SEGS * nq
    rows = tok // n_head
    chunk = tok // CHUNKS
    vmem = pl.BlockSpec(memory_space=pltpu.VMEM)
    smem = pl.BlockSpec(memory_space=pltpu.SMEM)
    hop = pltpu.VMEM((2, CHUNKS, chunk, D), BF16)
    sems = pltpu.SemaphoreType.DMA((2, 2, 2, CHUNKS))
    width = group * BT
    hbm = pl.BlockSpec(memory_space=pl.ANY)
    landed = pl.pallas_call(
        functools.partial(kernel, n_ctx, n_head, tok, group),
        out_shape=(
            jax.ShapeDtypeStruct((n_head, rows, qw), BF16),
            jax.ShapeDtypeStruct((n_head, rows, D), BF16),
            jax.ShapeDtypeStruct((n_head, rows, D), BF16),
        ),
        in_specs=[hbm] * 4 + [vmem, smem],
        out_specs=(hbm,) * 3,
        scratch_shapes=[
            pltpu.VMEM((nq, group, BT, D), BF16),
            pltpu.VMEM((nq, group, BT, D), BF16),
            pltpu.VMEM((2, 8, width), F32),
            pltpu.VMEM((8, BT), jnp.int32),
            pltpu.SMEM((8, BT), jnp.int32),
            pltpu.VMEM((nw + 1, BT, D), BF16),
            pltpu.VMEM((nw + 1, BT, D), BF16),
            pltpu.VMEM((2, SLOTS, BT, width), F32),
            pltpu.VMEM((nq, SLOTS, BT, width), BF16),
            pltpu.VMEM((nq, width, D), BF16),
            pltpu.VMEM((nq, 8, width), F32),
            pltpu.VMEM((nq, SLOTS + 1, BT, D), F32),
            pltpu.VMEM((nq, SLOTS + 1, BT, D), F32),
            pltpu.VMEM((tok, qw), BF16),
            hop, hop, hop, hop, hop, hop, hop, hop,
            pltpu.VMEM((tok, D), BF16),
            pltpu.VMEM((tok, D), BF16),
            sems, sems, sems, sems,
            pltpu.SemaphoreType.DMA((3, n_head)),
            pltpu.SemaphoreType.DMA((3, n_head)),
            pltpu.SemaphoreType.DMA((8,)),
            pltpu.SemaphoreType.DMA((2, group)),
        ],
        compiler_params=pltpu.CompilerParams(
            collective_id=0, has_side_effects=True, vmem_limit_bytes=60 * 1024 * 1024
        ),
    )(
        queries.reshape(nq, BT, qw), keys.reshape(nq, BT, D), values.reshape(nq, BT, D),
        output_gradient.reshape(nq, BT, qw), blocks, counts,
    )
    return pl.pallas_call(
        assemble,
        out_shape=(
            jax.ShapeDtypeStruct((rows, n_head * qw), BF16),
            jax.ShapeDtypeStruct((rows, n_head * D), BF16),
            jax.ShapeDtypeStruct((rows, n_head * D), BF16),
        ),
        in_specs=[vmem] * 3,
        out_specs=(vmem,) * 3,
    )(*landed)


def solution(mesh):
    return jax.shard_map(
        functools.partial(on_device, mesh.shape["ctx"], mesh.shape["head"]),
        mesh=mesh,
        in_specs=(
            P("ctx", "head"),
            P("ctx", "head"),
            P("ctx", "head"),
            P("ctx", "head"),
            P("ctx", None),
            P("ctx"),
        ),
        out_specs=(P(("ctx", "head"), None), P(("ctx", "head"), None), P(("ctx", "head"), None)),
        check_vma=False,
    )
```
